32 devices in a mesh: ctx: 8 (over y, x, core), wsh: 4 (over z).
Axes of the slice: x: 2, y: 2, z: 4, core: 2. Of those that a mesh axis runs over, the one named last changes fastest.
Arguments:
- tokens: bfloat16 [4, 1024, 1792], P('wsh', 'ctx'), may hold values from -6 to 6
- cotangent: bfloat16 [4, 1024, 1792], P('wsh', 'ctx'), may hold values from -6 to 6
- segment_ids: int32 [4, 1024], P('wsh'), may hold values from 0 to 23, never falling along the last dimension, each value on 1 to 256 neighbouring positions
- block_order: int32 [16], replicated, may hold values from 0 to 15, as said below
- premix: float32 [1792], P(('ctx', 'wsh')), may hold values from 0.5 to 1.5
- inward: float32 [1792, 2304], P(('ctx', 'wsh')), may hold values from -0.125 to 0.125
- filters: float32 [3, 1792], P(None, ('ctx', 'wsh')), may hold values from -4 to 4
- outward: float32 [1792, 1792], P(('ctx', 'wsh')), may hold values from -1 to 1
- prefeed: float32 [1792], P(('ctx', 'wsh')), may hold values from 0.5 to 1.5
- expand: float32 [1792, 9728], P(('ctx', 'wsh')), may hold values from -0.125 to 0.125
- shrink: float32 [4864, 1792], P(('ctx', 'wsh')), may hold values from -0.078125 to 0.078125
- premix_state: float32 [2, 1792], P(None, ('ctx', 'wsh')), may hold values from -30 to 100, as said below
- inward_state: float32 [2, 1792, 2304], P(None, ('ctx', 'wsh')), may hold values from -30 to 100, as said below
- filters_state: float32 [2, 3, 1792], P(None, None, ('ctx', 'wsh')), may hold values from -30 to 100, as said below
- outward_state: float32 [2, 1792, 1792], P(None, ('ctx', 'wsh')), may hold values from -30 to 100, as said below
- prefeed_state: float32 [2, 1792], P(None, ('ctx', 'wsh')), may hold values from -30 to 100, as said below
- expand_state: float32 [2, 1792, 9728], P(None, ('ctx', 'wsh')), may hold values from -30 to 100, as said below
- shrink_state: float32 [2, 4864, 1792], P(None, ('ctx', 'wsh')), may hold values from -30 to 100, as said below
Outputs:
- block_output: bfloat16 [4, 1024, 1792], P('wsh', 'ctx')
- input_grad: bfloat16 [4, 1024, 1792], P('wsh', 'ctx')
- premix_grad: float32 [1792], P(('ctx', 'wsh'))
- inward_grad: float32 [1792, 2304], P(('ctx', 'wsh'))
- filters_grad: float32 [3, 1792], P(None, ('ctx', 'wsh'))
- outward_grad: float32 [1792, 1792], P(('ctx', 'wsh'))
- prefeed_grad: float32 [1792], P(('ctx', 'wsh'))
- expand_grad: float32 [1792, 9728], P(('ctx', 'wsh'))
- shrink_grad: float32 [4864, 1792], P(('ctx', 'wsh'))
- premix_moments: float32 [2, 1792], P(None, ('ctx', 'wsh'))
- inward_moments: float32 [2, 1792, 2304], P(None, ('ctx', 'wsh'))
- filters_moments: float32 [2, 3, 1792], P(None, None, ('ctx', 'wsh'))
- outward_moments: float32 [2, 1792, 1792], P(None, ('ctx', 'wsh'))
- prefeed_moments: float32 [2, 1792], P(None, ('ctx', 'wsh'))
- expand_moments: float32 [2, 1792, 9728], P(None, ('ctx', 'wsh'))
- shrink_moments: float32 [2, 4864, 1792], P(None, ('ctx', 'wsh'))
- premix_master: float32 [1792], P(('ctx', 'wsh'))
- inward_master: float32 [1792, 2304], P(('ctx', 'wsh'))
- filters_master: float32 [3, 1792], P(None, ('ctx', 'wsh'))
- outward_master: float32 [1792, 1792], P(('ctx', 'wsh'))
- prefeed_master: float32 [1792], P(('ctx', 'wsh'))
- expand_master: float32 [1792, 9728], P(('ctx', 'wsh'))
- shrink_master: float32 [4864, 1792], P(('ctx', 'wsh'))
- weight_norms: float32 [2, 7], replicated
The draws below stay inside these ranges and needn't reach their ends.
Inputs may be any that keep to these rules, and one draw needn't show every extreme that they name: `segment_ids`: each sequence's segment numbers never fall along positions and start at 0; a segment holds at most 256 positions and one holds exactly that many. `block_order`: A permutation of the 16 blocks; the two slots of each index of ctx hold blocks b and 15 - b for some b. `premix_state`: index 0 holds first moments, index 1 second moments, which are positive. `inward_state`: index 0 holds first moments, index 1 second moments, which are positive. `filters_state`: index 0 holds first moments, index 1 second moments, which are positive. `outward_state`: index 0 holds first moments, index 1 second moments, which are positive. `prefeed_state`: index 0 holds first moments, index 1 second moments, which are positive. `expand_state`: index 0 holds first moments, index 1 second moments, which are positive. `shrink_state`: index 0 holds first moments, index 1 second moments, which are positive.
All inputs are finite; a program needn't handle non-finite values.
Results may differ from the reference program's by a relative error of at most 0.013.
The reference program's roundings to bfloat16 on the way count: a program that leaves them out, or rounds other values in their place, can miss the bound.
Values may be sent and summed in bfloat16 or wider, within the bound.
A program may use at most 320 MiB of HBM per device.

```python
import math
import jax
import jax.numpy as jnp
import numpy as np
from jax import lax

D = 1792
FF = 4864
HEADS = 16
QUERY_KEY_WIDTH = 16
KCONV = 3
STEP = 3
BLK = 64
HDV = 112
QK = 256
NBLK = 16
LEN = 1024
SEQS = 4


def moment_draw(key, array_shape, marker):
    own_key = jax.random.fold_in(key, marker)
    first_moment = 5.0 * jnp.clip(jax.random.normal(jax.random.fold_in(own_key, 11), array_shape, jnp.float32), -6.0, 6.0)
    second = jnp.exp(jax.random.uniform(jax.random.fold_in(own_key, 12), array_shape, jnp.float32, math.log(5.0), math.log(100.0)))
    return jnp.stack([first_moment, second])


def draw_premix_state(key, part):
    return moment_draw(key, (D,), 101)


def draw_inward_state(key, part):
    return moment_draw(key, (D, 2 * QK + D), 102)


def draw_filters_state(key, part):
    return moment_draw(key, (KCONV, D), 103)


def draw_outward_state(key, part):
    return moment_draw(key, (D, D), 104)


def draw_prefeed_state(key, part):
    return moment_draw(key, (D,), 105)


def draw_expand_state(key, part):
    return moment_draw(key, (D, 2 * FF), 106)


def draw_shrink_state(key, part):
    return moment_draw(key, (FF, D), 107)


def draw_block_order(key, part):
    paired = NBLK // 2
    early = jax.random.permutation(jax.random.fold_in(key, 21), paired).astype(jnp.int32)
    flips = jax.random.randint(jax.random.fold_in(key, 22), (paired,), 0, 2)
    late = NBLK - 1 - early
    leading = jnp.where(flips == 1, late, early)
    trailing = jnp.where(flips == 1, early, late)
    return jnp.stack([leading, trailing], axis=1).reshape(NBLK).astype(jnp.int32)


def level_of(key, dims, pieces, least, high):
    factor_of = 1.0
    for position, blocks in pieces:
        draws = jax.random.uniform(jax.random.fold_in(jax.random.fold_in(key, 6), position), (blocks,), jnp.float32, least / len(pieces), high / len(pieces))
        factor_of = factor_of * jnp.repeat(jnp.exp(draws), dims[position] // blocks).reshape((-1,) + (1,) * (len(dims) - 1 - position))
    return factor_of


def profile(amount, total, bound, skew):
    weights = [(1 << 20) // math.isqrt(grade ** skew) + 1 for grade in range(2, amount + 1)]
    surplus, counts = total - bound - (amount - 1), [1] * (amount - 1)
    while surplus > 0:
        free = [i for i in range(amount - 1) if counts[i] < bound]
        whole, remaining = sum([weights[i] for i in free]), surplus
        for i in free:
            extra = min(bound - counts[i], max(1, remaining * weights[i] // whole), surplus)
            counts[i] = counts[i] + extra
            surplus = surplus - extra
    return np.array([bound] + counts)


def uneven_parts(rng, count, total, bound, skew):
    if count == 2:
        one = jax.random.randint(rng, (), max(1, total - bound), min(bound, total - 1) + 1)
        return jnp.stack([one, total - one])
    tallies = jnp.asarray(profile(count, total, bound, skew), jnp.int32)
    twos = (count - 1) // 2
    giver, receiver = tallies[1:1 + 2 * twos:2], tallies[2:2 + 2 * twos:2]
    room = jnp.minimum(giver - 1, bound - receiver)
    passed = jax.random.randint(jax.random.fold_in(rng, 1), (twos,), 0, 1 << 20) % (room + 1)
    tallies = tallies.at[1:1 + 2 * twos:2].set(giver - passed).at[2:2 + 2 * twos:2].set(receiver + passed)
    return tallies[jax.random.permutation(jax.random.fold_in(rng, 2), count)]


def gaussian(key, shape, scale, bound, cuts=(), held_as=jnp.bfloat16):
    level = level_of(key, shape, cuts, -0.22, 0.18) if cuts else 1.0
    values = jax.random.normal(key, shape, jnp.float32) * scale * level
    return jnp.minimum(jnp.maximum(values, -bound), bound).astype(held_as)


def setup_inputs(seed: int = 0) -> dict:
    keys = jax.random.split(jax.random.key(seed), 19)
    tokens = gaussian(keys[0], (SEQS, LEN, D), 1.0, 6.0, ((0, 4), (1, 8)))
    cotangent = gaussian(keys[1], (SEQS, LEN, D), 1.0, 6.0, ((0, 4), (1, 8)))
    segment_ids = jax.vmap(lambda own: jnp.searchsorted(jnp.cumsum(uneven_parts(own, 24, LEN, LEN // 4, 3)), jnp.arange(LEN), side="right"))(jax.random.split(keys[2], SEQS)).reshape((SEQS, LEN)).astype(jnp.int32)
    block_order = draw_block_order(jax.random.fold_in(keys[18], 71), 0)
    premix = jnp.clip(1.0 + 0.1 * jax.random.normal(keys[4], (D,), jnp.float32), 0.5, 1.5)
    inward = gaussian(keys[5], (D, 2 * QK + D), D ** -0.5, 0.125, ((0, 32),), jnp.float32)
    filters = gaussian(keys[6], (KCONV, D), 0.6, 4.0, ((1, 32),), jnp.float32)
    outward = gaussian(keys[7], (D, D), (D // 64) ** -0.5, 1.0, ((0, 32),), jnp.float32)
    prefeed = jnp.clip(1.0 + 0.1 * jax.random.normal(keys[8], (D,), jnp.float32), 0.5, 1.5)
    expand = gaussian(keys[9], (D, 2 * FF), D ** -0.5, 0.125, ((0, 32),), jnp.float32)
    shrink = gaussian(keys[10], (FF, D), FF ** -0.5, 0.078125, ((0, 32),), jnp.float32)
    premix_state = draw_premix_state(jax.random.fold_in(keys[18], 71), 0)
    inward_state = draw_inward_state(jax.random.fold_in(keys[18], 71), 0)
    filters_state = draw_filters_state(jax.random.fold_in(keys[18], 71), 0)
    outward_state = draw_outward_state(jax.random.fold_in(keys[18], 71), 0)
    prefeed_state = draw_prefeed_state(jax.random.fold_in(keys[18], 71), 0)
    expand_state = draw_expand_state(jax.random.fold_in(keys[18], 71), 0)
    shrink_state = draw_shrink_state(jax.random.fold_in(keys[18], 71), 0)
    return dict(tokens=tokens, cotangent=cotangent, segment_ids=segment_ids, block_order=block_order, premix=premix, inward=inward, filters=filters, outward=outward, prefeed=prefeed, expand=expand, shrink=shrink, premix_state=premix_state, inward_state=inward_state, filters_state=filters_state, outward_state=outward_state, prefeed_state=prefeed_state, expand_state=expand_state, shrink_state=shrink_state)


@jax.custom_vjp
def low(v):
    return lax.optimization_barrier(v.astype(jnp.bfloat16)).astype(jnp.float32)

@jax.custom_vjp
def low_back(v):
    return v

def low_keep(v):
    return (low(v), None)

def low_pass(kept, grad):
    return (grad,)

def back_keep(v):
    return (v, None)

def back_low(kept, grad):
    return (low(grad),)
low.defvjp(low_keep, low_pass)
low_back.defvjp(back_keep, back_low)
norm_eps = 1e-05
adam_eps = 1e-08
beta_first = 0.9
beta_second = 0.99
learn_rate = 0.5
highest_precision = lax.Precision.HIGHEST

def matmul(left, right):
    return jnp.dot(left, right, precision=highest_precision, preferred_element_type=jnp.float32)

def rms_scale(values):
    return values * lax.rsqrt(lax.optimization_barrier(jnp.mean(values * values, axis=-1, keepdims=True)) + norm_eps)

def sequence_forward(params, inputs, segments):
    premix, inward, filters, outward, prefeed, expand, shrink = params
    normed_one = low(rms_scale(inputs) * low(premix))
    project = low_back(matmul(normed_one, low(inward)))
    queries = low(project[:, :QK]).reshape(LEN, HEADS, QUERY_KEY_WIDTH)
    key_collection = low(project[:, QK:2 * QK]).reshape(LEN, HEADS, QUERY_KEY_WIDTH)
    valueset = low(project[:, 2 * QK:])
    taps_low = low(filters)
    positions = jnp.arange(LEN, dtype=jnp.int32)
    convolved = jnp.zeros((LEN, D), jnp.float32)
    for offset in range(KCONV):
        source = jnp.maximum(positions - offset, 0)
        usable = ((positions - offset >= 0) & (jnp.take(segments, source) == segments)).astype(jnp.float32)
        convolved = convolved + taps_low[offset] * (jnp.take(valueset, source, axis=0) * usable[:, None])
    head_values = valueset.reshape(LEN, HEADS, HDV)
    row_span = min(512, LEN)

    def query_block(start_row):
        query_block_rows = lax.dynamic_slice_in_dim(queries, start_row, row_span, 0)
        block_pos = start_row + jnp.arange(row_span, dtype=jnp.int32)
        block_seg = lax.dynamic_slice_in_dim(segments, start_row, row_span, 0)
        attention_scores = low_back(jnp.einsum('rwb,nwb->wrn', query_block_rows, key_collection, precision=highest_precision) * QUERY_KEY_WIDTH ** (-0.5))
        allowed = ((positions[None, :] <= block_pos[:, None]) & (segments[None, :] == block_seg[:, None])).astype(jnp.float32)
        weights = (1.0 + attention_scores + 0.5 * attention_scores * attention_scores) * allowed[None]
        totals = lax.optimization_barrier(jnp.sum(weights, axis=2))
        numerator = low_back(jnp.einsum('hqk,khd->qhd', low(weights), head_values, precision=highest_precision))
        return (numerator / jnp.transpose(totals)[:, :, None]).reshape(row_span, D)
    starts = (jnp.arange(LEN // row_span) * row_span).astype(jnp.int32)
    attended = lax.map(jax.checkpoint(query_block), starts).reshape(LEN, D)
    gated = low(attended * jax.nn.silu(convolved))
    residual = inputs + low_back(matmul(gated, low(outward)))
    normed_two = low(rms_scale(residual) * low(prefeed))
    gate_up = low_back(matmul(normed_two, low(expand)))
    activated = low(jax.nn.silu(gate_up[:, :FF]) * gate_up[:, FF:])
    return residual + low_back(matmul(activated, low(shrink)))

def reference(tokens, cotangent, segment_ids, block_order, premix, inward, filters, outward, prefeed, expand, shrink, premix_state, inward_state, filters_state, outward_state, prefeed_state, expand_state, shrink_state):
    params = (premix, inward, filters, outward, prefeed, expand, shrink)
    states = (premix_state, inward_state, filters_state, outward_state, prefeed_state, expand_state, shrink_state)
    inverse = jnp.zeros((NBLK,), jnp.int32).at[block_order].set(jnp.arange(NBLK, dtype=jnp.int32))

    def to_natural(values):
        return values.reshape(SEQS, NBLK, BLK, D)[:, inverse].reshape(SEQS, LEN, D)

    def to_dealt(values):
        return values.reshape(SEQS, NBLK, BLK, D)[:, block_order].reshape(SEQS, LEN, D)
    inputs = to_natural(tokens.astype(jnp.float32))
    grad_out = to_natural(cotangent.astype(jnp.float32))

    def one_sequence(running, sequence_items):
        seq_input, seq_grad, seq_segments = sequence_items
        result, pullback = jax.vjp(lambda weights, values: sequence_forward(weights, values, seq_segments), params, seq_input)
        weight_grads, input_grads = pullback(seq_grad)
        running = tuple((left + right for left, right in zip(running, weight_grads)))
        return (running, (result, input_grads))
    zeroed = tuple((jnp.zeros_like(weight) for weight in params))
    gradients, (results, input_grads) = lax.scan(one_sequence, zeroed, (inputs, grad_out, segment_ids))
    block_output = to_dealt(results).astype(jnp.bfloat16)
    input_grad = to_dealt(input_grads).astype(jnp.bfloat16)
    moments = []
    masters = []
    weight_list = []
    step_list = []
    for weight, state_pair, gradient in zip(params, states, gradients):
        first_moment = beta_first * state_pair[0] + (1.0 - beta_first) * gradient
        second = beta_second * state_pair[1] + (1.0 - beta_second) * gradient * gradient
        direction = first_moment / (1.0 - beta_first ** STEP) / (jnp.sqrt(second / (1.0 - beta_second ** STEP)) + adam_eps)
        weight_norm = jnp.sqrt(jnp.sum(weight * weight))
        step_norm = jnp.sqrt(jnp.sum(direction * direction))
        moments.append(jnp.stack([first_moment, second]))
        masters.append(weight - learn_rate * (weight_norm / step_norm) * direction)
        weight_list.append(weight_norm)
        step_list.append(step_norm)
    weight_norms = jnp.stack([jnp.stack(weight_list), jnp.stack(step_list)])
    return (block_output, input_grad, gradients[0], gradients[1], gradients[2], gradients[3], gradients[4], gradients[5], gradients[6], moments[0], moments[1], moments[2], moments[3], moments[4], moments[5], moments[6], masters[0], masters[1], masters[2], masters[3], masters[4], masters[5], masters[6], weight_norms)
```

```python
import jax
import jax.numpy as jnp
from jax import lax
from jax.sharding import PartitionSpec as P

HEADS = 16
QUERY_KEY_WIDTH = 16
KCONV = 3
STEP = 3
HDV = 112
QK = 256
TILE = 128

norm_eps = 1e-05
adam_eps = 1e-08
beta_first = 0.9
beta_second = 0.99
learn_rate = 0.5

f32 = jnp.float32
bf16 = jnp.bfloat16
BOTH = ("ctx", "wsh")


def mm(left, right):
    return jnp.dot(left, right, preferred_element_type=f32)


def mm_nt(left, right):
    return lax.dot_general(left, right, (((1,), (1,)), ((), ())), preferred_element_type=f32)


def mm_tn(left, right):
    return lax.dot_general(left, right, (((0,), (0,)), ((), ())), preferred_element_type=f32)


def inverse_rms(values):
    return lax.rsqrt(jnp.mean(values * values, axis=-1, keepdims=True) + norm_eps)


def rms_back(grad_normed, normed, scaler):
    return scaler * (grad_normed - normed * jnp.mean(grad_normed * normed, axis=-1, keepdims=True))


def silu_slope(values):
    sigmoid = jax.nn.sigmoid(values)
    return sigmoid * (1.0 + values * (1.0 - sigmoid))


def gather_rows(values):
    return lax.all_gather(values, "ctx", axis=0, tiled=True)


def scatter_sum(values, ctx):
    rows, columns = values.shape
    pieces = lax.all_to_all(values.reshape(ctx, rows // ctx, columns), "ctx", 0, 0)
    return jnp.sum(pieces.astype(f32), axis=0)


def split_columns(shard, parts, ctx):
    rows = shard.shape[0]
    pieces, start = [], 0
    for width in parts:
        piece = shard[:, start : start + width].reshape(rows, ctx, width // ctx)
        pieces.append(piece)
        start += width
    return jnp.transpose(jnp.concatenate(pieces, axis=2), (1, 0, 2))


def join_columns(pieces, parts, ctx):
    moved = jnp.transpose(pieces, (1, 0, 2))
    rows, joined, start = moved.shape[0], [], 0
    for width in parts:
        own = width // ctx
        joined.append(moved[:, :, start : start + own].reshape(rows, width))
        start += own
    return jnp.concatenate(joined, axis=1)


def gather_columns(shard, parts, ctx):
    pieces = split_columns(shard, parts, ctx)
    rows, columns = pieces.shape[1:]
    swapped = lax.all_to_all(pieces, "ctx", 0, 0)
    full = lax.all_gather(swapped, "wsh", axis=1)
    return full.reshape(-1, columns)


def return_columns(grad, parts, ctx, wsh):
    columns = grad.shape[1]
    pieces = grad.astype(bf16).reshape(ctx, wsh, -1, columns)
    swapped = lax.all_to_all(pieces, "wsh", 1, 0)
    summed = jnp.sum(swapped.astype(f32), axis=0).astype(bf16)
    back = lax.all_to_all(summed, "ctx", 0, 0)
    return join_columns(back, parts, ctx).astype(f32)


def return_rows(grad, wsh):
    columns = grad.shape[1]
    pieces = grad.astype(bf16).reshape(wsh, -1, columns)
    swapped = lax.all_to_all(pieces, "wsh", 0, 0)
    return jnp.sum(swapped.astype(f32), axis=0)


def windows(values, prior):
    tiles = values.reshape((-1, TILE) + values.shape[1:])
    count = tiles.shape[0]
    padded = jnp.concatenate([jnp.zeros((prior,) + tiles.shape[1:], values.dtype), tiles], axis=0)
    return jnp.concatenate([padded[j : j + count] for j in range(prior + 1)], axis=1)


def unwindow(grads, prior):
    count = grads.shape[0]
    tail = grads.shape[2:]
    pieces = grads.reshape((count, prior + 1, TILE) + tail)
    total = jnp.zeros((count + prior, TILE) + tail, grads.dtype)
    for j in range(prior + 1):
        total = total.at[j : j + count].add(pieces[:, j])
    return total[prior:].reshape((count * TILE,) + tail)


def scores_of(query_tiles, key_windows, allowed):
    scores = jnp.einsum(
        "tqhd,tkhd->htqk", query_tiles, key_windows, preferred_element_type=f32
    ) * (QUERY_KEY_WIDTH ** (-0.5))
    return scores, (1.0 + scores + 0.5 * scores * scores) * allowed[None]


def allowed_of(segments, prior):
    length = segments.shape[0]
    positions = jnp.arange(length, dtype=jnp.int32)
    key_pos = jnp.arange(length, dtype=jnp.int32) + 1
    key_windows = windows(key_pos, prior)
    seg_windows = windows(segments, prior)
    pos_tiles = positions.reshape(-1, TILE)
    seg_tiles = segments.reshape(-1, TILE)
    return (
        (key_windows[:, None, :] >= 1)
        & (key_windows[:, None, :] - 1 <= pos_tiles[:, :, None])
        & (seg_windows[:, None, :] == seg_tiles[:, :, None])
    ).astype(f32)


def shifted(values, offset):
    if offset == 0:
        return values
    rows = values.shape[0]
    edge = jnp.zeros((abs(offset),) + values.shape[1:], values.dtype)
    if offset > 0:
        return jnp.concatenate([edge, values[: rows - offset]], axis=0)
    return jnp.concatenate([values[-offset:], edge], axis=0)


def make_body(ctx, wsh):
    def body(
        tokens, cotangent, segment_ids, block_order,
        premix, inward, filters, outward, prefeed, expand, shrink,
        premix_state, inward_state, filters_state, outward_state,
        prefeed_state, expand_state, shrink_state,
    ):
        masters = (premix, inward, filters, outward, prefeed, expand, shrink)
        states = (
            premix_state, inward_state, filters_state, outward_state,
            prefeed_state, expand_state, shrink_state,
        )
        width = tokens.shape[2]
        feed = expand.shape[1] // 2
        segments = segment_ids[0]
        length = segments.shape[0]
        blocks = block_order.shape[0]
        block_rows = length // blocks
        prior = -(-(length // 4 - 1) // TILE)
        heads = HEADS // ctx
        keys_width = QK // ctx
        own_values = width // ctx
        own_feed = feed // ctx
        inverse = (
            jnp.zeros((blocks,), jnp.int32).at[block_order].set(jnp.arange(blocks, dtype=jnp.int32))
        )

        def reorder(values, indices):
            return jnp.take(values.reshape(blocks, block_rows, -1), indices, axis=0).reshape(
                length, -1
            )

        in_parts, ex_parts = (QK, QK, width), (feed, feed)
        gains = lax.all_gather(
            jnp.stack([premix, prefeed]).astype(bf16), BOTH, axis=1, tiled=True
        ).astype(f32)
        gain_one, gain_two = gains[0], gains[1]
        taps = lax.all_gather(filters.astype(bf16), "wsh", axis=1, tiled=True).astype(f32)
        inward_own = gather_columns(inward.astype(bf16), in_parts, ctx)
        outward_own = lax.all_gather(outward.astype(bf16), "wsh", axis=0, tiled=True)
        expand_own = gather_columns(expand.astype(bf16), ex_parts, ctx)
        shrink_own = lax.all_gather(shrink.astype(bf16), "wsh", axis=0, tiled=True)
        tokens_all = gather_rows(tokens[0])
        grad_ffn = gather_rows(cotangent[0])

        inputs_all = tokens_all.astype(f32)
        mixed_in = (inputs_all * inverse_rms(inputs_all) * gain_one).astype(bf16)
        project = reorder(mm(mixed_in, inward_own).astype(bf16), inverse)
        queries = project[:, :keys_width].reshape(-1, TILE, heads, QUERY_KEY_WIDTH)
        keys = project[:, keys_width : 2 * keys_width].reshape(length, heads, QUERY_KEY_WIDTH)
        values = project[:, 2 * keys_width :]
        value_float = values.astype(f32)
        usable, tapped = [], []
        for offset in range(KCONV):
            usable.append(
                (
                    (shifted(segments, offset) == segments)
                    & (jnp.arange(length) >= offset)
                ).astype(f32)[:, None]
            )
            tapped.append(shifted(value_float, offset) * usable[offset])
        convolved = sum(taps[offset] * tapped[offset] for offset in range(KCONV))
        allowed = allowed_of(segments, prior)
        key_windows = windows(keys, prior)
        value_windows = windows(values.reshape(length, heads, HDV), prior)
        scores, weights = scores_of(queries, key_windows, allowed)
        probs = weights.astype(bf16)
        totals = jnp.sum(weights, axis=3)
        totals_rows = jnp.transpose(totals, (1, 2, 0))[..., None]
        numer = jnp.einsum("htqk,tkhd->tqhd", probs, value_windows, preferred_element_type=f32)
        attended = numer / totals_rows
        attended_flat = attended.reshape(length, own_values)
        conv_gate = jax.nn.silu(convolved)
        gated = reorder((attended_flat * conv_gate).astype(bf16), block_order)
        mixed_out = mm(gated, outward_own).astype(bf16)
        inputs = tokens[0].astype(f32)
        residual = inputs + scatter_sum(mixed_out, ctx)
        scaler_two = inverse_rms(residual)
        normed_two = residual * scaler_two
        feed_in = gather_rows((normed_two * gain_two).astype(bf16))

        gate_up = mm(feed_in, expand_own)
        gate_part, up_part = gate_up[:, :own_feed], gate_up[:, own_feed:]
        gate_silu = jax.nn.silu(gate_part)
        activated = (gate_silu * up_part).astype(bf16)
        block_output = (
            residual + scatter_sum(mm(activated, shrink_own).astype(bf16), ctx)
        ).astype(bf16)
        shrink_grad = mm_tn(activated, grad_ffn)
        grad_act = mm_nt(grad_ffn, shrink_own)
        grad_gate_up = jnp.concatenate(
            [grad_act * up_part * silu_slope(gate_part), grad_act * gate_silu], axis=1
        ).astype(bf16)
        expand_grad = mm_tn(feed_in, grad_gate_up)
        grad_feed = scatter_sum(mm_nt(grad_gate_up, expand_own).astype(bf16), ctx)
        prefeed_part = jnp.sum(grad_feed * normed_two, axis=0)
        grad_resid = cotangent[0].astype(f32) + rms_back(
            grad_feed * gain_two, normed_two, scaler_two
        )
        grad_mix = gather_rows(grad_resid.astype(bf16))

        outward_grad = mm_tn(gated, grad_mix)
        grad_gated = reorder(mm_nt(grad_mix, outward_own), inverse)
        grad_attended = (grad_gated * conv_gate).reshape(-1, TILE, heads, HDV)
        grad_conv = grad_gated * attended_flat * silu_slope(convolved)
        filters_part = jnp.stack(
            [jnp.sum(grad_conv * tapped[offset], axis=0) for offset in range(KCONV)]
        )
        grad_numer = (grad_attended / totals_rows).astype(bf16)
        grad_totals = -jnp.sum(grad_attended * attended, axis=3) / totals_rows[..., 0]
        grad_totals = jnp.transpose(grad_totals, (2, 0, 1))
        grad_weights = (
            jnp.einsum("tqhd,tkhd->htqk", grad_numer, value_windows, preferred_element_type=f32)
            + grad_totals[..., None]
        )
        score_gradient = (grad_weights * (1.0 + scores) * allowed[None]).astype(bf16)
        scale = QUERY_KEY_WIDTH ** (-0.5)
        grad_query = (
            jnp.einsum("htqk,tkhd->tqhd", score_gradient, key_windows, preferred_element_type=f32)
            * scale
        )
        grad_keys = (
            unwindow(
                jnp.einsum("htqk,tqhd->tkhd", score_gradient, queries, preferred_element_type=f32),
                prior,
            )
            * scale
        )
        grad_values = unwindow(
            jnp.einsum("htqk,tqhd->tkhd", probs, grad_numer, preferred_element_type=f32), prior
        ).reshape(length, own_values)
        for offset in range(KCONV):
            grad_values = grad_values + taps[offset] * shifted(
                grad_conv * usable[offset], -offset
            )
        grad_project = reorder(
            jnp.concatenate(
                [
                    grad_query.reshape(length, keys_width),
                    grad_keys.reshape(length, keys_width),
                    grad_values,
                ],
                axis=1,
            ).astype(bf16),
            block_order,
        )
        inward_grad = mm_tn(mixed_in, grad_project)
        grad_mixin = scatter_sum(mm_nt(grad_project, inward_own).astype(bf16), ctx)
        scaler_one = inverse_rms(inputs)
        normed_one = inputs * scaler_one
        premix_part = jnp.sum(grad_mixin * normed_one, axis=0)
        input_grad = (
            grad_resid + rms_back(grad_mixin * gain_one, normed_one, scaler_one)
        ).astype(bf16)

        gain_grads = lax.psum_scatter(
            jnp.stack([premix_part, prefeed_part]), BOTH, scatter_dimension=1, tiled=True
        )
        shards = (
            gain_grads[0],
            return_columns(inward_grad, in_parts, ctx, wsh),
            lax.psum_scatter(filters_part, "wsh", scatter_dimension=1, tiled=True),
            return_rows(outward_grad, wsh),
            gain_grads[1],
            return_columns(expand_grad, ex_parts, ctx, wsh),
            return_rows(shrink_grad, wsh),
        )
        return (block_output[None], input_grad[None]) + shards + update(masters, states, shards)

    return body


def update(masters, states, shards):
    moments = []
    directions = []
    for state_pair, gradient in zip(states, shards):
        first_moment = beta_first * state_pair[0] + (1.0 - beta_first) * gradient
        second = beta_second * state_pair[1] + (1.0 - beta_second) * gradient * gradient
        directions.append(
            first_moment
            / (1.0 - beta_first**STEP)
            / (jnp.sqrt(second / (1.0 - beta_second**STEP)) + adam_eps)
        )
        moments.append(jnp.stack([first_moment, second]))
    step_sums = jnp.stack([jnp.sum(direction * direction) for direction in directions])
    weight_sums = jnp.stack([jnp.sum(weight * weight) for weight in masters])
    totals = lax.psum(jnp.stack([weight_sums, step_sums]), BOTH)
    norms = jnp.sqrt(totals)
    updated = [
        masters[i] - learn_rate * (norms[0, i] / norms[1, i]) * directions[i] for i in range(7)
    ]
    return tuple(moments) + tuple(updated) + (norms,)


def solution(mesh):
    ctx, wsh = mesh.shape["ctx"], mesh.shape["wsh"]
    rows, columns, moments_rows = P(BOTH, None), P(None, BOTH), P(None, BOTH, None)
    vector, whole = P(BOTH), P("wsh", "ctx", None)
    weights = (vector, rows, columns, rows, vector, rows, rows)
    states = (
        columns, moments_rows, P(None, None, BOTH), moments_rows,
        columns, moments_rows, moments_rows,
    )
    return jax.shard_map(
        make_body(ctx, wsh),
        mesh=mesh,
        in_specs=(whole, whole, P("wsh", None), P()) + weights + states,
        out_specs=(whole, whole) + weights + states + weights + (P(),),
        check_vma=False,
    )
```
